128 devices in a mesh: gx: 4 (over x), gy: 4 (over y_hi, core), gz: 8 (over z, y_lo).
Axes of the slice: x: 4, y: 4 (y_hi: 2, y_lo: 2; y = y_hi * 2 + y_lo), z: 4, core: 2. Of those that a mesh axis runs over, the one named last changes fastest.
Arguments:
- field: bfloat16 [1, 64, 16, 32, 1024], P(None, None, 'gx', 'gy', 'gz'), may hold values from -6 to 6
- kernel_one: bfloat16 [3, 3, 3, 64, 64], replicated, may hold values from -0.15625 to 0.15625
- bias_one: float32 [64], replicated, may hold values from -3 to 3
- kernel_two: bfloat16 [3, 3, 3, 64, 64], replicated, may hold values from -0.15625 to 0.15625
- bias_two: float32 [64], replicated, may hold values from -3 to 3
- kernel_three: bfloat16 [3, 3, 3, 64, 64], replicated, may hold values from -0.15625 to 0.15625
- bias_three: float32 [64], replicated, may hold values from -3 to 3
Outputs:
- latent: bfloat16 [1, 64, 16, 32, 1024], P(None, None, 'gx', 'gy', 'gz')
The draws below stay inside these ranges and needn't reach their ends.
All inputs are finite; a program needn't handle non-finite values.
Results may differ from the reference program's by a relative error of at most 0.0048.
Values may be sent and summed in bfloat16 or wider, within the bound.
A program may use at most 256 MiB of HBM per device.

```python
import jax
import jax.numpy as jnp

C = 64
B = 1
NX = 16
NY = 32
NZ = 1024


def shard_levels(key, dims, cuts, low, top_value):
    factor_of = 1.0
    for dim, blocks in cuts:
        steps = jax.random.uniform(jax.random.fold_in(jax.random.fold_in(key, 6), dim), (blocks,), jnp.float32, low / len(cuts), top_value / len(cuts))
        factor_of = factor_of * jnp.repeat(jnp.exp(steps), dims[dim] // blocks).reshape((-1,) + (1,) * (len(dims) - 1 - dim))
    return factor_of


def gaussian(stream_key, shape, deviation, reach, shards=(), dtype=jnp.bfloat16):
    entries = jax.random.normal(stream_key, shape, jnp.float32) * deviation
    if len(shards) > 0:
        entries = shard_levels(stream_key, shape, shards, -0.22, 0.18) * entries
    return jnp.clip(entries, min=-reach, max=reach).astype(dtype)


def setup_inputs(seed: int = 0) -> dict:
    arg_keys = jax.random.split(jax.random.key(seed), 8)
    return {
        "field": gaussian(arg_keys[0], (B, C, NX, NY, NZ), 1.0, 6.0, ((2, 4), (3, 4), (4, 8))),
        "kernel_one": gaussian(arg_keys[1], (3, 3, 3, C, C), (27 * C) ** -0.5, 0.15625),
        "bias_one": gaussian(arg_keys[2], (C,), 0.5, 3.0, (), jnp.float32),
        "kernel_two": gaussian(arg_keys[3], (3, 3, 3, C, C), (27 * C) ** -0.5, 0.15625),
        "bias_two": gaussian(arg_keys[4], (C,), 0.5, 3.0, (), jnp.float32),
        "kernel_three": gaussian(arg_keys[5], (3, 3, 3, C, C), (27 * C) ** -0.5, 0.15625),
        "bias_three": gaussian(arg_keys[6], (C,), 0.5, 3.0, (), jnp.float32),
    }


def layer(values, kernel, bias):
    total = jnp.zeros(values.shape, jnp.float32)
    for along_x in range(3):
        for along_y in range(3):
            for along_z in range(3):
                shifted = jnp.roll(values, (1 - along_x, 1 - along_y, 1 - along_z), axis=(2, 3, 4))
                matrix = kernel[along_x, along_y, along_z].astype(jnp.float32)
                total = total + jnp.einsum("oc,bcxyz->boxyz", matrix, shifted)
    total = total + bias.astype(jnp.float32)[None, :, None, None, None]
    return jax.nn.gelu(total, approximate=False).astype(jnp.bfloat16)


def reference(field, kernel_one, bias_one, kernel_two, bias_two, kernel_three, bias_three):
    first = layer(field.astype(jnp.float32), kernel_one, bias_one)
    second = layer(first.astype(jnp.float32), kernel_two, bias_two)
    return layer(second.astype(jnp.float32), kernel_three, bias_three)
```

```python
import functools

import jax
import jax.numpy as jnp
from jax import lax
from jax.experimental import pallas as pl
from jax.experimental.pallas import tpu as pltpu
from jax.sharding import PartitionSpec as P

MESH = pl.DeviceIdType.MESH
AXES = ("gx", "gy", "gz")
HALF = 64
LX, LY, LP = 4, 8, 64
FLAT = [(dx, dy, 0) for dx in (-1, 0, 1) for dy in (-1, 0, 1) if (dx, dy) != (0, 0)]
SIDES = [(dx, dy, dz) for dz in (-1, 1) for dx in (-1, 0, 1) for dy in (-1, 0, 1)]
WAYS = FLAT + SIDES


def neighbour(way):
    ids = []
    for axis, step in zip(AXES, way):
        count = lax.axis_size(axis)
        ids.append(lax.rem(lax.axis_index(axis) + step + count, count))
    return tuple(ids)


def message(layer, way, a, zs, zr, send, recv):
    dx, dy, dz = way
    which = WAYS.index(way)
    if dz == 0:
        near_x = {1: LX, -1: 1, 0: pl.ds(1, LX)}[dx]
        far_x = {1: 0, -1: LX + 1, 0: pl.ds(1, LX)}[dx]
        near_y = {1: LY, -1: 1, 0: pl.ds(1, LY)}[dy]
        far_y = {1: 0, -1: LY + 1, 0: pl.ds(1, LY)}[dy]
        source = a.at[layer, near_x, near_y]
        target = a.at[layer, far_x, far_y]
    else:
        side, other = (1, 0) if dz == 1 else (0, 1)
        source = zs.at[layer, side]
        target = zr.at[layer, other, 1 - dx, 1 - dy]
        if dx != 0:
            plane = LX - 1 if dx == 1 else 0
            source = source.at[plane]
            target = target.at[plane]
    return pltpu.make_async_remote_copy(
        src_ref=source,
        dst_ref=target,
        send_sem=send.at[layer, which],
        recv_sem=recv.at[layer, which],
        device_id=neighbour(way),
        device_id_type=MESH,
    )


def kernel(field, weights, bias, out, a, b, zs, zr, edge, halo, send, recv, local):
    load = pltpu.make_async_copy(field, a.at[0, pl.ds(1, LX), pl.ds(1, LY)], local)
    load.start()
    barrier = pltpu.get_barrier_semaphore()
    for way in WAYS:
        pl.semaphore_signal(barrier, inc=1, device_id=neighbour(way), device_id_type=MESH)
    load.wait()

    lane = lax.broadcasted_iota(jnp.int32, (LP, 2 * HALF), 1)
    row = lax.broadcasted_iota(jnp.int32, (LP, 2 * HALF), 0)
    even = lane < HALF
    ends = (even & (row == LP - 1)) | (~even & (row == 0))
    even_row = lax.broadcasted_iota(jnp.int32, (LY, 2 * HALF), 1) < HALF

    def pack_edges(layer):
        for side in range(2):
            for x in range(LX):
                zs[layer, side, x] = edge[side, x].astype(jnp.bfloat16)

    def first_edges(i, carry):
        x, y = i // LY, i % LY
        slab = a[0, x + 1, y + 1].astype(jnp.float32)
        edge[0, x, pl.ds(y, 1), :] = slab[0:1]
        edge[1, x, pl.ds(y, 1), :] = slab[LP - 1 :]
        return carry

    lax.fori_loop(0, LX * LY, first_edges, 0)
    pack_edges(0)
    pl.semaphore_wait(barrier, len(WAYS))

    def copies(layer):
        return [message(layer, way, a, zs, zr, send, recv) for way in WAYS]

    for copy in copies(0):
        copy.start()

    for layer in range(3):
        for copy in copies(layer):
            copy.wait_recv()

        for x in range(LX + 2):
            ix = 0 if x == 0 else 2 if x == LX + 1 else 1
            sx = (x - 1) % LX
            for iy in range(3):
                rows = jnp.where(
                    even_row,
                    zr[layer, 1, ix, iy, sx].astype(jnp.float32),
                    zr[layer, 0, ix, iy, sx].astype(jnp.float32),
                )
                if iy == 0:
                    halo[x, 7:8, :] = rows[7:8]
                elif iy == 1:
                    halo[x, 8:16, :] = rows
                else:
                    halo[x, 16:17, :] = rows[0:1]

        def shift(i, carry):
            x, y = i // (LY + 2), i % (LY + 2)
            slab = a[layer, x, y].astype(jnp.float32)
            up = pltpu.roll(slab, LP - 1, 0)
            down = pltpu.roll(slab, 1, 0)
            fill = jnp.broadcast_to(halo[x, pl.ds(y + 7, 1), :], (LP, 2 * HALF))
            b[x, y] = jnp.where(ends, fill, jnp.where(even, up, down)).astype(jnp.bfloat16)
            return carry

        lax.fori_loop(0, (LX + 2) * (LY + 2), shift, 0)

        def plane(x):
            total = None
            for along_x in range(3):
                for t in range(4):
                    left = jnp.concatenate([a[layer, x + along_x, t + 2 * j] for j in range(LY // 2)], axis=0)
                    right = jnp.concatenate([b[x + along_x, t + 2 * j] for j in range(LY // 2)], axis=0)
                    term = jnp.dot(
                        jnp.concatenate([left, right], axis=1),
                        jnp.concatenate([weights[layer, along_x, t + 1], weights[layer, along_x, t]], axis=1),
                        preferred_element_type=jnp.float32,
                    )
                    total = term if total is None else total + term
            total = total + bias[layer]
            value = 0.5 * total * (1.0 + lax.erf(total * 0.7071067811865476))
            for j in range(LY // 2):
                for side in range(2):
                    y = 2 * j + side
                    slab = value[j * LP : (j + 1) * LP, side * 2 * HALF : (side + 1) * 2 * HALF]
                    if layer < 2:
                        a[layer + 1, x + 1, y + 1] = slab.astype(jnp.bfloat16)
                        edge[0, x, y : y + 1, :] = slab[0:1]
                        edge[1, x, y : y + 1, :] = slab[LP - 1 :]
                    else:
                        out[x, y] = slab.astype(jnp.bfloat16)

        def outer(i, carry):
            plane(i * (LX - 1))
            return carry

        def inner(i, carry):
            plane(i + 1)
            return carry

        lax.fori_loop(0, 2, outer, 0)
        if layer < 2:
            for side in range(2):
                for x in (0, LX - 1):
                    zs[layer + 1, side, x] = edge[side, x].astype(jnp.bfloat16)
            for way in WAYS:
                if way[0] != 0:
                    message(layer + 1, way, a, zs, zr, send, recv).start()
        lax.fori_loop(0, 2, inner, 0)
        if layer < 2:
            for side in range(2):
                for x in range(1, LX - 1):
                    zs[layer + 1, side, x] = edge[side, x].astype(jnp.bfloat16)
            for way in WAYS:
                if way[0] == 0:
                    message(layer + 1, way, a, zs, zr, send, recv).start()

    for layer in range(3):
        for copy in copies(layer):
            copy.wait_send()


def toeplitz(weight):
    taps = jnp.transpose(weight, (0, 1, 2, 4, 3))
    zero = jnp.zeros_like(taps[:, :, 0])
    first, middle, last = taps[:, :, 0], taps[:, :, 1], taps[:, :, 2]
    lower = jnp.concatenate([middle, last, zero, first], axis=2)
    upper = jnp.concatenate([first, middle, last, zero], axis=2)
    block = jnp.concatenate([lower, upper], axis=3)
    return jnp.pad(block, ((0, 0), (1, 1), (0, 0), (0, 0)))


def shards(field, kernel_one, bias_one, kernel_two, bias_two, kernel_three, bias_three):
    channels = field.shape[1]
    cells = field.reshape(channels, LX, LY, LP, 2)
    cells = jnp.transpose(cells, (1, 2, 3, 4, 0)).reshape(LX, LY, LP, 2 * channels)
    weights = jnp.stack([toeplitz(k) for k in (kernel_one, kernel_two, kernel_three)])
    bias = jnp.stack([jnp.tile(v, 4)[None] for v in (bias_one, bias_two, bias_three)])
    vmem = pl.BlockSpec(memory_space=pltpu.VMEM)
    result = pl.pallas_call(
        kernel,
        out_shape=jax.ShapeDtypeStruct((LX, LY, LP, 2 * HALF), jnp.bfloat16),
        in_specs=[pl.BlockSpec(memory_space=pl.ANY), vmem, vmem],
        out_specs=vmem,
        scratch_shapes=[
            pltpu.VMEM((3, LX + 2, LY + 2, LP, 2 * HALF), jnp.bfloat16),
            pltpu.VMEM((LX + 2, LY + 2, LP, 2 * HALF), jnp.bfloat16),
            pltpu.VMEM((3, 2, LX, LY, 2 * HALF), jnp.bfloat16),
            pltpu.VMEM((3, 2, 3, 3, LX, LY, 2 * HALF), jnp.bfloat16),
            pltpu.VMEM((2, LX, LY, 2 * HALF), jnp.float32),
            pltpu.VMEM((LX + 2, 24, 2 * HALF), jnp.float32),
            pltpu.SemaphoreType.DMA((3, len(WAYS))),
            pltpu.SemaphoreType.DMA((3, len(WAYS))),
            pltpu.SemaphoreType.DMA,
        ],
        compiler_params=pltpu.CompilerParams(
            collective_id=0, has_side_effects=True, vmem_limit_bytes=48 * 1024 * 1024
        ),
    )(cells, weights, bias)
    result = result.reshape(LX, LY, LP, 2, channels)
    return jnp.transpose(result, (4, 0, 1, 2, 3)).reshape(1, channels, LX, LY, 2 * LP)


def solution(mesh):
    return jax.shard_map(
        shards,
        mesh=mesh,
        in_specs=(P(None, None, "gx", "gy", "gz"), P(), P(), P(), P(), P(), P()),
        out_specs=P(None, None, "gx", "gy", "gz"),
        check_vma=False,
    )
```

```python
import jax
import jax.numpy as jnp
from jax import lax
from jax.experimental import pallas as pl
from jax.experimental.pallas import tpu as pltpu
from jax.sharding import PartitionSpec as P

MESH = pl.DeviceIdType.MESH
AXES = ("gx", "gy", "gz")
C = 64
W = 2 * C
LX, LY, LP = 4, 8, 64
LZ = 2 * LP
PAIRS = LY // 2
INNER, OUTER = "inner", "outer"
BF = jnp.bfloat16
F32 = jnp.float32


def plan():
    entries = []
    for dx in (-1, 1):
        entries.append(((dx, 0, 0), OUTER, None))
        for dy in (-1, 1):
            entries.append(((dx, dy, 0), OUTER, None))
    for dz in (-1, 1):
        for dx in (-1, 1, 0):
            for dy in (-1, 0, 1):
                entries.append(((dx, dy, dz), OUTER, None))
    for dy in (-1, 1):
        entries.append(((0, dy, 0), OUTER, (1, 1)))
        entries.append(((0, dy, 0), OUTER, (LX, 1)))
        entries.append(((0, dy, 0), INNER, (2, LX - 2)))
    return entries


PLAN = plan()
WAYS = sorted({way for way, _, _ in PLAN})


def neighbour(way):
    ids = []
    for axis, step in zip(AXES, way):
        count = lax.axis_size(axis)
        ids.append(lax.rem(lax.axis_index(axis) + step + count, count))
    return tuple(ids)


def message(layer, which, a, zs, zr, send, recv):
    (dx, dy, dz), _, planes = PLAN[which]
    if dz == 0:
        across = pl.ds(*planes) if dx == 0 else None
        near_x = {1: LX, -1: 1, 0: across}[dx]
        far_x = {1: 0, -1: LX + 1, 0: across}[dx]
        near_y = {1: LY, -1: 1, 0: pl.ds(1, LY)}[dy]
        far_y = {1: 0, -1: LY + 1, 0: pl.ds(1, LY)}[dy]
        source = a.at[layer, near_x, near_y]
        target = a.at[layer, far_x, far_y]
    else:
        side, other = (1, 0) if dz == 1 else (0, 1)
        source = zs.at[layer, side]
        target = zr.at[layer, other, 1 - dx, 1 - dy]
        if dx != 0:
            plane = LX - 1 if dx == 1 else 0
            source = source.at[plane]
            target = target.at[plane]
    return pltpu.make_async_remote_copy(
        src_ref=source,
        dst_ref=target,
        send_sem=send.at[layer, which],
        recv_sem=recv.at[layer, which],
        device_id=neighbour((dx, dy, dz)),
        device_id_type=MESH,
    )


def kernel(
    field, k_one, k_two, k_three, b_one, b_two, b_three, out,
    raw, wide, taps, weights, bias, spread, gather, a, b, zs, zr, edge, halo, stage, thin,
    send, recv, field_sem, tap_sem, out_sem, bias_sem,
):
    field_in = [pltpu.make_async_copy(field.at[0, :, x], raw.at[x], field_sem.at[x]) for x in range(LX)]
    taps_in = [pltpu.make_async_copy(k, taps.at[i], tap_sem.at[i]) for i, k in enumerate((k_one, k_two, k_three))]
    for x in (0, LX - 1, *range(1, LX - 1)):
        field_in[x].start()
    bias_in = [pltpu.make_async_copy(v, thin.at[i], bias_sem.at[i]) for i, v in enumerate((b_one, b_two, b_three))]
    for copy in taps_in + bias_in:
        copy.start()
    barrier = pltpu.get_barrier_semaphore()
    for way in WAYS:
        pl.semaphore_signal(barrier, inc=1, device_id=neighbour(way), device_id_type=MESH)

    def one_hot(natural, paired):
        slab, z = natural // LZ, natural % LZ
        parity, other, pair = paired // W, (paired // LP) % 2, paired % LP
        return ((slab == other) & (z == 2 * pair + parity)).astype(F32).astype(BF)

    first = lax.broadcasted_iota(jnp.int32, (2 * LZ, 2 * W), 0)
    second = lax.broadcasted_iota(jnp.int32, (2 * LZ, 2 * W), 1)
    spread[...] = one_hot(first, second)
    gather[...] = one_hot(second, first)

    def relay_in(x):
        field_in[x].wait()
        wide[...] = raw[x].astype(F32).reshape(C * LY, LZ)
        rows = []
        for j in range(PAIRS):
            pair = [wide[pl.ds(2 * j + s, C, stride=LY), :].astype(BF) for s in range(2)]
            rows.append(jnp.concatenate(pair, axis=1))
        split = jnp.dot(jnp.concatenate(rows, axis=0), spread[...], preferred_element_type=F32).astype(BF)
        for j in range(PAIRS):
            block = split[j * C : (j + 1) * C]
            cells = jnp.concatenate([block[:, :W], block[:, W:]], axis=0).T
            for s in range(2):
                y = 2 * j + s
                slab = cells[s * LP : (s + 1) * LP]
                a[0, x + 1, y + 1] = slab
                edge[0, x, y : y + 1, :] = slab[:16].astype(F32)[:1]
                edge[1, x, y : y + 1, :] = slab[LP - 16 :].astype(F32)[15:]

    def pack_edges(layer, planes):
        for side in range(2):
            for x in planes:
                zs[layer, side, x] = edge[side, x].astype(BF)

    def start(layer, choose):
        for which, entry in enumerate(PLAN):
            if choose(entry):
                message(layer, which, a, zs, zr, send, recv).start()

    def arrive(layer, choose):
        for which, entry in enumerate(PLAN):
            if choose(entry):
                message(layer, which, a, zs, zr, send, recv).wait_recv()

    def crosses_x(entry):
        return entry[0][0] != 0

    def stays_outer(entry):
        return entry[0][0] == 0 and entry[1] == OUTER

    def stays_inner(entry):
        return entry[0][0] == 0 and entry[1] == INNER

    outer_planes = (0, LX - 1)
    inner_planes = tuple(range(1, LX - 1))

    for x in outer_planes:
        relay_in(x)
    pack_edges(0, outer_planes)
    pl.semaphore_wait(barrier, len(WAYS))
    start(0, crosses_x)
    for x in inner_planes:
        relay_in(x)
    pack_edges(0, inner_planes)
    start(0, stays_outer)
    start(0, stays_inner)

    none = jnp.zeros((C, C), BF)
    for layer in range(3):
        taps_in[layer].wait()
        bias_in[layer].wait()
        twice = jnp.concatenate([thin[layer], thin[layer]], axis=1)
        bias[layer] = jnp.concatenate([twice, twice], axis=1)

        def band(i, carry):
            along_x, along_y = i // 3, i % 3
            tap = [taps[layer, along_x, along_y, f] for f in range(3)]
            order = ((tap[1], tap[0]), (tap[2], tap[1]), (none, tap[2]), (tap[0], none))
            for k, (low, high) in enumerate(order):
                block = jnp.concatenate([low, high], axis=0).T
                weights[layer, i, k * C : (k + 1) * C, :] = block
            return carry

        lax.fori_loop(0, 9, band, 0)

    lane = lax.broadcasted_iota(jnp.int32, (LP, W), 1)
    row = lax.broadcasted_iota(jnp.int32, (LP, W), 0)
    even = lane < C
    ends = (even & (row == LP - 1)) | (~even & (row == 0))
    even_row = lax.broadcasted_iota(jnp.int32, (LY, W), 1) < C
    blank = jnp.zeros((2 * W, W), BF)

    for layer in range(3):

        def shift(x, ix, sx):
            for iy in range(3):
                rows = jnp.where(even_row, zr[layer, 1, ix, iy, sx].astype(F32), zr[layer, 0, ix, iy, sx].astype(F32))
                if iy == 0:
                    halo[7:8, :] = rows[7:8]
                elif iy == 1:
                    halo[8:16, :] = rows
                else:
                    halo[16:17, :] = rows[0:1]
            for y in range(LY + 2):
                slab = a[layer, x, y].astype(F32)
                up = pltpu.roll(slab, LP - 1, 0)
                down = pltpu.roll(slab, 1, 0)
                fill = jnp.broadcast_to(halo[y + 7 : y + 8, :], (LP, W))
                b[x, y] = jnp.where(ends, fill, jnp.where(even, up, down)).astype(BF)

        def shift_local(i, carry):
            shift(i + 1, 1, i)
            return carry

        def plane(x):
            total = None
            for along_x in range(3):
                for t in range(4):
                    left = jnp.concatenate([a[layer, x + along_x, t + 2 * j] for j in range(PAIRS)], axis=0)
                    right = jnp.concatenate([b[x + along_x, t + 2 * j] for j in range(PAIRS)], axis=0)
                    low = weights[layer, 3 * along_x + t] if t < 3 else blank
                    high = weights[layer, 3 * along_x + t - 1] if t > 0 else blank
                    term = jnp.dot(
                        jnp.concatenate([left, right], axis=1),
                        jnp.concatenate([low, high], axis=1),
                        preferred_element_type=F32,
                    )
                    total = term if total is None else total + term
            total = total + bias[layer]
            value = 0.5 * total * (1.0 + lax.erf(total * 0.7071067811865476))
            if layer < 2:
                for j in range(PAIRS):
                    for s in range(2):
                        y = 2 * j + s
                        slab = value[j * LP : (j + 1) * LP, s * W : (s + 1) * W]
                        a[layer + 1, x + 1, y + 1] = slab.astype(BF)
                        edge[0, x, y : y + 1, :] = slab[0:1]
                        edge[1, x, y : y + 1, :] = slab[LP - 1 :]
            else:
                rounded = value.astype(BF)
                rows = []
                for j in range(PAIRS):
                    block = rounded[j * LP : (j + 1) * LP]
                    turned = jnp.concatenate([block[:, :W], block[:, W:]], axis=0).T
                    rows.append(jnp.concatenate([turned[:C], turned[C:]], axis=1))
                merged = jnp.dot(jnp.concatenate(rows, axis=0), gather[...], preferred_element_type=F32)
                for j in range(PAIRS):
                    for s in range(2):
                        wide[pl.ds(2 * j + s, C, stride=LY), :] = merged[j * C : (j + 1) * C, s * LZ : (s + 1) * LZ]
                stage[x] = wide[...].reshape(C, LY, LZ).astype(BF)
                pltpu.make_async_copy(stage.at[x], out.at[0, :, x], out_sem.at[x]).start()

        arrive(layer, lambda entry: not crosses_x(entry))
        lax.fori_loop(0, LX, shift_local, 0)
        for x in inner_planes:
            plane(x)
        if layer < 2:
            pack_edges(layer + 1, inner_planes)
            start(layer + 1, stays_inner)
        arrive(layer, crosses_x)
        shift(0, 0, LX - 1)
        shift(LX + 1, 2, 0)
        for x in outer_planes:
            plane(x)
        if layer < 2:
            pack_edges(layer + 1, outer_planes)
            start(layer + 1, crosses_x)
            start(layer + 1, stays_outer)

    for layer in range(3):
        for which in range(len(PLAN)):
            message(layer, which, a, zs, zr, send, recv).wait_send()
    for x in range(LX):
        pltpu.make_async_copy(stage.at[x], out.at[0, :, x], out_sem.at[x]).wait()


def shards(field, kernel_one, bias_one, kernel_two, bias_two, kernel_three, bias_three):
    hbm = pl.BlockSpec(memory_space=pltpu.HBM)
    return pl.pallas_call(
        kernel,
        out_shape=jax.ShapeDtypeStruct(field.shape, BF),
        in_specs=[hbm] * 7,
        out_specs=hbm,
        scratch_shapes=[
            pltpu.VMEM((LX, C, LY, LZ), BF),
            pltpu.VMEM((C * LY, LZ), F32),
            pltpu.VMEM((3, 3, 3, 3, C, C), BF),
            pltpu.VMEM((3, 9, 2 * W, W), BF),
            pltpu.VMEM((3, 1, 2 * W), F32),
            pltpu.VMEM((2 * LZ, 2 * W), BF),
            pltpu.VMEM((2 * W, 2 * LZ), BF),
            pltpu.VMEM((3, LX + 2, LY + 2, LP, W), BF),
            pltpu.VMEM((LX + 2, LY + 2, LP, W), BF),
            pltpu.VMEM((3, 2, LX, LY, W), BF),
            pltpu.VMEM((3, 2, 3, 3, LX, LY, W), BF),
            pltpu.VMEM((2, LX, LY, W), F32),
            pltpu.VMEM((24, W), F32),
            pltpu.VMEM((LX, C, LY, LZ), BF),
            pltpu.VMEM((3, 1, C), F32),
            pltpu.SemaphoreType.DMA((3, len(PLAN))),
            pltpu.SemaphoreType.DMA((3, len(PLAN))),
            pltpu.SemaphoreType.DMA((LX,)),
            pltpu.SemaphoreType.DMA((3,)),
            pltpu.SemaphoreType.DMA((LX,)),
            pltpu.SemaphoreType.DMA((3,)),
        ],
        compiler_params=pltpu.CompilerParams(
            collective_id=0, has_side_effects=True, vmem_limit_bytes=65_900_000
        ),
    )(
        field,
        kernel_one,
        kernel_two,
        kernel_three,
        bias_one.reshape(1, C),
        bias_two.reshape(1, C),
        bias_three.reshape(1, C),
    )


def solution(mesh):
    return jax.shard_map(
        shards,
        mesh=mesh,
        in_specs=(P(None, None, "gx", "gy", "gz"), P(), P(), P(), P(), P(), P()),
        out_specs=P(None, None, "gx", "gy", "gz"),
        check_vma=False,
    )
```

```python
import jax
import jax.numpy as jnp
from jax import lax
from jax.experimental import pallas as pl
from jax.experimental.pallas import tpu as pltpu
from jax.sharding import PartitionSpec as P

MESH = pl.DeviceIdType.MESH
AXES = ("gx", "gy", "gz")
C = 64
W = 2 * C
LX, LY, LP = 4, 8, 64
LZ = 2 * LP
PAIRS = LY // 2
BF = jnp.bfloat16
F32 = jnp.float32
HIGH = {1: 1, -1: 0}


def plan():
    both = (-1, 1)
    entries = [((dx, dy, dz), 1, None) for dx in both for dy in both for dz in both]
    entries += [((dx, dy, 0), 1, None) for dx in both for dy in both]
    entries += [((0, dy, 0), 1, piece) for dy in both for piece in ((1, 1), (LX, 1))]
    entries += [((dx, 0, 0), 1, (1, 2)) for dx in both]
    entries += [((dx, 0, dz), 2, None) for dx in both for dz in both]
    entries += [((0, dy, dz), 2, None) for dy in both for dz in both]
    entries += [((0, 0, dz), 2, None) for dz in both]
    entries += [((dx, 0, 0), 2, (LY - 1, 2)) for dx in both]
    entries += [((0, dy, 0), 3, (2, LX - 2)) for dy in both]
    entries += [((dx, 0, 0), 4, (3, LY - 4)) for dx in both]
    return entries


PLAN = plan()
WAYS = sorted({way for way, _, _ in PLAN})


def neighbour(way):
    ids = []
    for axis, step in zip(AXES, way):
        count = lax.axis_size(axis)
        ids.append(lax.rem(lax.axis_index(axis) + step + count, count))
    return tuple(ids)


def message(layer, which, a, out_rows, in_rows, send, recv):
    (dx, dy, dz), _, piece = PLAN[which]
    if dz == 0:
        near_x = {1: LX, -1: 1}.get(dx)
        far_x = {1: 0, -1: LX + 1}.get(dx)
        near_y = {1: LY, -1: 1}.get(dy)
        far_y = {1: 0, -1: LY + 1}.get(dy)
        if dx == 0:
            near_x = far_x = pl.ds(*piece)
        if dy == 0:
            near_y = far_y = pl.ds(*piece)
        source = a.at[layer, near_x, near_y]
        target = a.at[layer, far_x, far_y]
    else:
        kind = (dx != 0) + 2 * (dy != 0)
        source = out_rows[kind].at[layer, HIGH[dz]]
        target = in_rows[kind].at[layer, HIGH[-dz]]
        for step in (dx, dy):
            if step != 0:
                source = source.at[HIGH[step]]
                target = target.at[HIGH[-step]]
    return pltpu.make_async_remote_copy(
        src_ref=source,
        dst_ref=target,
        send_sem=send.at[layer, which],
        recv_sem=recv.at[layer, which],
        device_id=neighbour((dx, dy, dz)),
        device_id_type=MESH,
    )


def kernel(
    field, k_one, k_two, k_three, b_one, b_two, b_three, out,
    raw, wide, taps, weights, bias, spread, gather, a, b,
    z_all, z_x, z_y, z_xy, r_all, r_x, r_y, r_xy, e_all, e_y, e_xy, halo, thin,
    send, recv, field_sem, tap_sem, bias_sem,
):
    out_rows = (z_all, z_x, z_y, z_xy)
    in_rows = (r_all, r_x, r_y, r_xy)
    field_in = [pltpu.make_async_copy(field.at[0, :, x], raw.at[x], field_sem.at[x]) for x in range(LX)]
    taps_in = [pltpu.make_async_copy(k, taps.at[i], tap_sem.at[i]) for i, k in enumerate((k_one, k_two, k_three))]
    for x in (0, LX - 1, *range(1, LX - 1)):
        field_in[x].start()
    bias_in = [pltpu.make_async_copy(v, thin.at[i], bias_sem.at[i]) for i, v in enumerate((b_one, b_two, b_three))]
    for copy in taps_in + bias_in:
        copy.start()
    barrier = pltpu.get_barrier_semaphore()
    for way in WAYS:
        pl.semaphore_signal(barrier, inc=1, device_id=neighbour(way), device_id_type=MESH)

    def one_hot(natural, paired):
        slab, z = natural // LZ, natural % LZ
        parity, other, pair = paired // W, (paired // LP) % 2, paired % LP
        return ((slab == other) & (z == 2 * pair + parity)).astype(F32).astype(BF)

    first = lax.broadcasted_iota(jnp.int32, (2 * LZ, 2 * W), 0)
    second = lax.broadcasted_iota(jnp.int32, (2 * LZ, 2 * W), 1)
    spread[...] = one_hot(first, second)
    gather[...] = one_hot(second, first)

    e_y[...] = jnp.zeros_like(e_y)
    e_xy[...] = jnp.zeros_like(e_xy)

    def keep_rows(x, y, rows):
        for side in range(2):
            e_all[side, x, y : y + 1, :] = rows[side]
            if y in (0, LY - 1):
                e_y[side, y // (LY - 1), x : x + 1, :] = rows[side]
                if x in (0, LX - 1):
                    e_xy[side, x // (LX - 1), y // (LY - 1), 0:1, :] = rows[side]

    def relay_in(x):
        field_in[x].wait()
        wide[x] = raw[x].astype(F32).reshape(C * LY, LZ)
        rows = []
        for j in range(PAIRS):
            pair = [wide[x, pl.ds(2 * j + s, C, stride=LY), :].astype(BF) for s in range(2)]
            rows.append(jnp.concatenate(pair, axis=1))
        split = jnp.dot(jnp.concatenate(rows, axis=0), spread[...], preferred_element_type=F32).astype(BF)
        for j in range(PAIRS):
            block = split[j * C : (j + 1) * C]
            cells = jnp.concatenate([block[:, :W], block[:, W:]], axis=0).T
            for s in range(2):
                y = 2 * j + s
                slab = cells[s * LP : (s + 1) * LP]
                a[0, x + 1, y + 1] = slab
                keep_rows(x, y, (slab[:16].astype(F32)[:1], slab[LP - 16 :].astype(F32)[15:]))

    def pack(layer, stage):
        for side in range(2):
            for i in range(2):
                if stage == 1:
                    for j in range(2):
                        z_xy[layer, side, i, j] = e_xy[side, i, j].astype(BF)
                elif stage == 2:
                    z_y[layer, side, i] = e_y[side, i].astype(BF)
                    z_x[layer, side, i] = e_all[side, i * (LX - 1)].astype(BF)
            if stage == 2:
                for x in range(LX):
                    z_all[layer, side, x] = e_all[side, x].astype(BF)

    def launch(layer, *stages):
        for stage in stages:
            pack(layer, stage)
        for which, entry in enumerate(PLAN):
            if entry[1] in stages:
                message(layer, which, a, out_rows, in_rows, send, recv).start()

    def arrive(layer, choose):
        for which, entry in enumerate(PLAN):
            if choose(entry):
                message(layer, which, a, out_rows, in_rows, send, recv).wait_recv()

    outer_planes, inner_planes = (0, LX - 1), tuple(range(1, LX - 1))
    outer_pairs, inner_pairs = (0, PAIRS - 1), tuple(range(1, PAIRS - 1))
    whole, middle = ((0, LP),), ((8, LP - 16),)

    def corner_of(planes, pairs):
        return [(x, j) for x in planes for j in pairs]

    for x in outer_planes:
        relay_in(x)
    pl.semaphore_wait(barrier, len(WAYS))
    launch(0, 1)
    for x in inner_planes:
        relay_in(x)
    launch(0, 2, 3, 4)

    none = jnp.zeros((C, C), BF)
    for layer in range(3):
        taps_in[layer].wait()
        bias_in[layer].wait()
        twice = jnp.concatenate([thin[layer], thin[layer]], axis=1)
        bias[layer] = jnp.concatenate([twice, twice], axis=1)

        def band(i, carry):
            along_x, along_y = i // 3, i % 3
            tap = [taps[layer, along_x, along_y, f] for f in range(3)]
            order = ((tap[1], tap[0]), (tap[2], tap[1]), (none, tap[2]), (tap[0], none))
            for k, (low, high) in enumerate(order):
                block = jnp.concatenate([low, high], axis=0).T
                weights[layer, i, k * C : (k + 1) * C, :] = block
            return carry

        lax.fori_loop(0, 9, band, 0)

    lane = lax.broadcasted_iota(jnp.int32, (LP, W), 1)
    row = lax.broadcasted_iota(jnp.int32, (LP, W), 0)
    even = lane < C
    top_row = (~even & (row == 0))[:8]
    low_row = (even & (row == LP - 1))[LP - 8 :]
    even_row = lax.broadcasted_iota(jnp.int32, (LY, W), 1) < C
    blank = jnp.zeros((2 * W, W), BF)

    def merge(ref, layer, *index):
        after, before = ref[(layer, 1, *index)], ref[(layer, 0, *index)]
        return jnp.where(even_row, after.astype(F32), before.astype(F32))

    def shift(layer, x, y):
        slab = a[layer, x, y].astype(F32)
        up = pltpu.roll(slab, LP - 1, 0)
        down = pltpu.roll(slab, 1, 0)
        b[x, y] = jnp.where(even, up, down).astype(BF)

    def patch(x, y):
        fill = jnp.broadcast_to(halo[x, y + 7 : y + 8, :], (8, W))
        top = b[x, y, 0:8, :].astype(F32)
        b[x, y, 0:8, :] = jnp.where(top_row, fill, top).astype(BF)
        low = b[x, y, LP - 8 : LP, :].astype(F32)
        b[x, y, LP - 8 : LP, :] = jnp.where(low_row, fill, low).astype(BF)

    def shift_own(layer):
        def step(i, carry):
            for y in range(LY):
                shift(layer, i + 1, y + 1)
            return carry

        lax.fori_loop(0, LX, step, 0)

    def finish_own(layer):
        for x in range(LX):
            halo[x + 1, 8:16, :] = merge(r_all, layer, x)
            for y in range(1, LY + 1):
                patch(x + 1, y)

    def finish_y(layer):
        for iy, y in enumerate((0, LY + 1)):
            rows = merge(r_y, layer, iy)
            for x in range(LX):
                halo[x + 1, y + 7 : y + 8, :] = rows[x : x + 1]
                shift(layer, x + 1, y)
                patch(x + 1, y)

    def finish_side(layer, ix):
        x = ix * (LX + 1)
        halo[x, 8:16, :] = merge(r_x, layer, ix)
        halo[x, 7:8, :] = merge(r_xy, layer, ix, 0)[0:1]
        halo[x, 16:17, :] = merge(r_xy, layer, ix, 1)[0:1]
        for y in range(LY + 2):
            shift(layer, x, y)
            patch(x, y)

    for layer in range(3):

        def block(places, spans):
            def rows_of(ref, *index):
                return [ref[(*index, pl.ds(low, size), slice(None))] for low, size in spans]

            depth = sum(size for _, size in spans)
            total = None
            for along_x in range(3):
                for t in range(4):
                    left, right = [], []
                    for x, j in places:
                        left += rows_of(a, layer, x + along_x, t + 2 * j)
                        right += rows_of(b, x + along_x, t + 2 * j)
                    low = weights[layer, 3 * along_x + t] if t < 3 else blank
                    high = weights[layer, 3 * along_x + t - 1] if t > 0 else blank
                    term = jnp.dot(
                        jnp.concatenate([jnp.concatenate(left, axis=0), jnp.concatenate(right, axis=0)], axis=1),
                        jnp.concatenate([low, high], axis=1),
                        preferred_element_type=F32,
                    )
                    total = term if total is None else total + term
            total = total + bias[layer]
            value = 0.5 * total * (1.0 + lax.erf(total * 0.7071067811865476))
            if layer < 2:
                for k, (x, j) in enumerate(places):
                    for s in range(2):
                        y = 2 * j + s
                        slab = value[k * depth : (k + 1) * depth, s * W : (s + 1) * W]
                        offset = 0
                        for low, size in spans:
                            a[layer + 1, x + 1, y + 1, low : low + size, :] = slab[offset : offset + size].astype(BF)
                            offset += size
                        if spans[0][0] == 0:
                            keep_rows(x, y, (slab[0:1], slab[depth - 1 :]))
            else:
                rounded = value.astype(BF)
                rows = []
                for k in range(len(places)):
                    part = rounded[k * LP : (k + 1) * LP]
                    turned = jnp.concatenate([part[:, :W], part[:, W:]], axis=0).T
                    rows.append(jnp.concatenate([turned[:C], turned[C:]], axis=1))
                merged = jnp.dot(jnp.concatenate(rows, axis=0), gather[...], preferred_element_type=F32)
                for k, (x, j) in enumerate(places):
                    for s in range(2):
                        wide[x, pl.ds(2 * j + s, C, stride=LY), :] = merged[k * C : (k + 1) * C, s * LZ : (s + 1) * LZ]

        shift_own(layer)
        arrive(layer, lambda entry: entry[0][:2] == (0, 0))
        finish_own(layer)
        if layer == 2:
            block(corner_of(inner_planes, inner_pairs), whole)
        arrive(layer, lambda entry: entry[0][0] == 0 and entry[0][1] != 0)
        finish_y(layer)
        if layer == 2:
            block(corner_of(inner_planes, outer_pairs), whole)
            for x in inner_planes:
                out[0, :, x] = wide[x].reshape(C, LY, LZ).astype(BF)
        arrive(layer, lambda entry: entry[0][0] != 0)
        for ix in range(2):
            finish_side(layer, ix)
        if layer < 2:
            block(corner_of(outer_planes, outer_pairs), whole)
            launch(layer + 1, 1)
            rest = corner_of(outer_planes, inner_pairs) + corner_of(inner_planes, range(PAIRS))
            block(rest, ((0, 8), (LP - 8, 8)))
            launch(layer + 1, 2)
            block(corner_of(inner_planes, outer_pairs), middle)
            launch(layer + 1, 3)
            block(corner_of(outer_planes, inner_pairs), middle)
            launch(layer + 1, 4)
            block(corner_of(inner_planes, inner_pairs), middle)
        else:
            block(corner_of(outer_planes, outer_pairs), whole)
            block(corner_of(outer_planes, inner_pairs), whole)
            for x in outer_planes:
                out[0, :, x] = wide[x].reshape(C, LY, LZ).astype(BF)

    for layer in range(3):
        for which in range(len(PLAN)):
            message(layer, which, a, out_rows, in_rows, send, recv).wait_send()


def shards(field, kernel_one, bias_one, kernel_two, bias_two, kernel_three, bias_three):
    hbm = pl.BlockSpec(memory_space=pltpu.HBM)
    operands = (
        field,
        kernel_one,
        kernel_two,
        kernel_three,
        bias_one.reshape(1, C),
        bias_two.reshape(1, C),
        bias_three.reshape(1, C),
    )
    return pl.pallas_call(
        kernel,
        out_shape=jax.ShapeDtypeStruct(field.shape, BF),
        in_specs=[hbm] * 7,
        out_specs=pl.BlockSpec(memory_space=pltpu.VMEM),
        scratch_shapes=[
            pltpu.VMEM((LX, C, LY, LZ), BF),
            pltpu.VMEM((LX, C * LY, LZ), F32),
            pltpu.VMEM((3, 3, 3, 3, C, C), BF),
            pltpu.VMEM((3, 9, 2 * W, W), BF),
            pltpu.VMEM((3, 1, 2 * W), F32),
            pltpu.VMEM((2 * LZ, 2 * W), BF),
            pltpu.VMEM((2 * W, 2 * LZ), BF),
            pltpu.VMEM((3, LX + 2, LY + 2, LP, W), BF),
            pltpu.VMEM((LX + 2, LY + 2, LP, W), BF),
            pltpu.VMEM((3, 2, LX, LY, W), BF),
            pltpu.VMEM((3, 2, 2, LY, W), BF),
            pltpu.VMEM((3, 2, 2, LY, W), BF),
            pltpu.VMEM((3, 2, 2, 2, LY, W), BF),
            pltpu.VMEM((3, 2, LX, LY, W), BF),
            pltpu.VMEM((3, 2, 2, LY, W), BF),
            pltpu.VMEM((3, 2, 2, LY, W), BF),
            pltpu.VMEM((3, 2, 2, 2, LY, W), BF),
            pltpu.VMEM((2, LX, LY, W), F32),
            pltpu.VMEM((2, 2, LY, W), F32),
            pltpu.VMEM((2, 2, 2, LY, W), F32),
            pltpu.VMEM((LX + 2, 24, W), F32),
            pltpu.VMEM((3, 1, C), F32),
            pltpu.SemaphoreType.DMA((3, len(PLAN))),
            pltpu.SemaphoreType.DMA((3, len(PLAN))),
            pltpu.SemaphoreType.DMA((LX,)),
            pltpu.SemaphoreType.DMA((3,)),
            pltpu.SemaphoreType.DMA((3,)),
        ],
        compiler_params=pltpu.CompilerParams(
            collective_id=0, has_side_effects=True, vmem_limit_bytes=48_000_000
        ),
    )(*[pltpu.with_memory_space_constraint(v, pltpu.HBM) for v in operands])


def solution(mesh):
    return jax.shard_map(
        shards,
        mesh=mesh,
        in_specs=(P(None, None, "gx", "gy", "gz"), P(), P(), P(), P(), P(), P()),
        out_specs=P(None, None, "gx", "gy", "gz"),
        check_vma=False,
    )
```

```python
import jax
import jax.numpy as jnp
from jax import lax
from jax.experimental import pallas as pl
from jax.experimental.pallas import tpu as pltpu
from jax.sharding import PartitionSpec as P

MESH = pl.DeviceIdType.MESH
AXES = ("gx", "gy", "gz")
C = 64
W = 2 * C
LX, LY, LP = 4, 8, 64
LZ = 2 * LP
PAIRS = LY // 2
BF = jnp.bfloat16
F32 = jnp.float32
HIGH = {1: 1, -1: 0}


LAST = (4, LY - 6)


def plan():
    both = (-1, 1)
    entries = [((0, dy, 0), 0, (2, LX - 2)) for dy in both]
    entries += [((dx, dy, dz), 1, None) for dx in both for dy in both for dz in both]
    entries += [((0, dy, dz), 1, None) for dy in both for dz in both]
    entries += [((dx, dy, 0), 1, None) for dx in both for dy in both]
    entries += [((0, dy, 0), 1, piece) for dy in both for piece in ((1, 1), (LX, 1))]
    entries += [((dx, 0, 0), 1, (1, 2)) for dx in both]
    entries += [((dx, 0, dz), 2, None) for dx in both for dz in both]
    entries += [((0, 0, dz), 2, None) for dz in both]
    entries += [((dx, 0, 0), 2, (LY - 1, 2)) for dx in both]
    entries += [((dx, 0, 0), 3, piece) for dx in both for piece in ((3, 1), (LY - 2, 1))]
    entries += [((dx, 0, 0), 3, LAST) for dx in both]
    return entries


PLAN = plan()
WAYS = sorted({way for way, _, _ in PLAN})


def neighbour(way):
    ids = []
    for axis, step in zip(AXES, way):
        count = lax.axis_size(axis)
        ids.append(lax.rem(lax.axis_index(axis) + step + count, count))
    return tuple(ids)


def message(layer, which, a, out_rows, in_rows, send, recv):
    (dx, dy, dz), _, piece = PLAN[which]
    if dz == 0:
        near_x = {1: LX, -1: 1}.get(dx)
        far_x = {1: 0, -1: LX + 1}.get(dx)
        near_y = {1: LY, -1: 1}.get(dy)
        far_y = {1: 0, -1: LY + 1}.get(dy)
        if dx == 0:
            near_x = far_x = pl.ds(*piece)
        if dy == 0:
            near_y = far_y = pl.ds(*piece)
        source = a.at[layer, near_x, near_y]
        target = a.at[layer, far_x, far_y]
    else:
        kind = (dx != 0) + 2 * (dy != 0)
        source = out_rows[kind].at[layer, HIGH[dz]]
        target = in_rows[kind].at[layer, HIGH[-dz]]
        for step in (dx, dy):
            if step != 0:
                source = source.at[HIGH[step]]
                target = target.at[HIGH[-step]]
    return pltpu.make_async_remote_copy(
        src_ref=source,
        dst_ref=target,
        send_sem=send.at[layer, which],
        recv_sem=recv.at[layer, which],
        device_id=neighbour((dx, dy, dz)),
        device_id_type=MESH,
    )


def kernel(
    field, k_one, k_two, k_three, b_one, b_two, b_three, out,
    raw, wide, taps, weights, bias, spread, gather, a, b,
    z_all, z_x, z_y, z_xy, r_all, r_x, r_y, r_xy, e_all, e_y, e_xy, halo, thin,
    send, recv, field_sem, tap_sem, bias_sem,
):
    out_rows = (z_all, z_x, z_y, z_xy)
    in_rows = (r_all, r_x, r_y, r_xy)
    barrier = pltpu.get_barrier_semaphore()
    for way in sorted(WAYS, key=lambda w: -sum(map(abs, w))):
        pl.semaphore_signal(barrier, inc=1, device_id=neighbour(way), device_id_type=MESH)
    field_in = [pltpu.make_async_copy(field.at[0, :, x], raw.at[x], field_sem.at[x]) for x in range(LX)]
    taps_in = [pltpu.make_async_copy(k, taps.at[i], tap_sem.at[i]) for i, k in enumerate((k_one, k_two, k_three))]
    for x in (0, LX - 1, *range(1, LX - 1)):
        field_in[x].start()
    bias_in = [pltpu.make_async_copy(v, thin.at[i], bias_sem.at[i]) for i, v in enumerate((b_one, b_two, b_three))]
    for copy in taps_in + bias_in:
        copy.start()

    def one_hot(natural, paired):
        slab, z = natural // LZ, natural % LZ
        parity, other, pair = paired // W, (paired // LP) % 2, paired % LP
        return ((slab == other) & (z == 2 * pair + parity)).astype(F32).astype(BF)

    first = lax.broadcasted_iota(jnp.int32, (2 * LZ, 2 * W), 0)
    second = lax.broadcasted_iota(jnp.int32, (2 * LZ, 2 * W), 1)
    spread[...] = one_hot(first, second)
    gather[...] = one_hot(second, first)

    e_y[...] = jnp.zeros_like(e_y)
    e_xy[...] = jnp.zeros_like(e_xy)

    def keep_rows(x, y, rows):
        for side in range(2):
            e_all[side, x, y : y + 1, :] = rows[side]
            if y in (0, LY - 1):
                e_y[side, y // (LY - 1), x : x + 1, :] = rows[side]
                if x in (0, LX - 1):
                    e_xy[side, x // (LX - 1), y // (LY - 1), 0:1, :] = rows[side]

    def relay_in(x):
        field_in[x].wait()
        wide[x] = raw[x].astype(F32).reshape(C * LY, LZ)
        rows = []
        for j in range(PAIRS):
            pair = [wide[x, pl.ds(2 * j + s, C, stride=LY), :].astype(BF) for s in range(2)]
            rows.append(jnp.concatenate(pair, axis=1))
        split = jnp.dot(jnp.concatenate(rows, axis=0), spread[...], preferred_element_type=F32).astype(BF)
        for j in range(PAIRS):
            block = split[j * C : (j + 1) * C]
            cells = jnp.concatenate([block[:, :W], block[:, W:]], axis=0).T
            for s in range(2):
                y = 2 * j + s
                slab = cells[s * LP : (s + 1) * LP]
                a[0, x + 1, y + 1] = slab
                keep_rows(x, y, (slab[:16].astype(F32)[:1], slab[LP - 16 :].astype(F32)[15:]))

    def pack(layer, stage):
        for side in range(2):
            for i in range(2):
                if stage == 1:
                    for j in range(2):
                        z_xy[layer, side, i, j] = e_xy[side, i, j].astype(BF)
                    z_y[layer, side, i] = e_y[side, i].astype(BF)
                elif stage == 2:
                    z_x[layer, side, i] = e_all[side, i * (LX - 1)].astype(BF)
            if stage == 2:
                for x in range(LX):
                    z_all[layer, side, x] = e_all[side, x].astype(BF)

    def launch(layer, *stages):
        for stage in stages:
            pack(layer, stage)
        for which, entry in enumerate(PLAN):
            if entry[1] in stages:
                message(layer, which, a, out_rows, in_rows, send, recv).start()

    def arrive(layer, choose):
        for which, entry in enumerate(PLAN):
            if choose(entry):
                message(layer, which, a, out_rows, in_rows, send, recv).wait_recv()

    outer_planes, inner_planes = (0, LX - 1), tuple(range(1, LX - 1))
    outer_pairs, inner_pairs = (0, PAIRS - 1), tuple(range(1, PAIRS - 1))
    whole, middle = ((0, LP),), ((8, LP - 16),)

    def corner_of(planes, pairs):
        return [(x, j) for x in planes for j in pairs]

    for x in outer_planes:
        relay_in(x)
    for x in inner_planes:
        relay_in(x)
    pl.semaphore_wait(barrier, len(WAYS))
    for stage in (1, 0, 2, 3):
        launch(0, stage)

    none = jnp.zeros((C, C), BF)
    for layer in range(3):
        taps_in[layer].wait()
        bias_in[layer].wait()
        twice = jnp.concatenate([thin[layer], thin[layer]], axis=1)
        bias[layer] = jnp.concatenate([twice, twice], axis=1)

        def band(i, carry):
            along_x, along_y = i // 3, i % 3
            tap = [taps[layer, along_x, along_y, f] for f in range(3)]
            order = ((tap[1], tap[0]), (tap[2], tap[1]), (none, tap[2]), (tap[0], none))
            for k, (low, high) in enumerate(order):
                block = jnp.concatenate([low, high], axis=0).T
                weights[layer, i, k * C : (k + 1) * C, :] = block
            return carry

        lax.fori_loop(0, 9, band, 0)

    lane = lax.broadcasted_iota(jnp.int32, (LP, W), 1)
    row = lax.broadcasted_iota(jnp.int32, (LP, W), 0)
    even = lane < C
    top_row = (~even & (row == 0))[:8]
    low_row = (even & (row == LP - 1))[LP - 8 :]
    even_row = lax.broadcasted_iota(jnp.int32, (LY, W), 1) < C
    blank = jnp.zeros((2 * W, W), BF)

    def merge(ref, layer, *index):
        after, before = ref[(layer, 1, *index)], ref[(layer, 0, *index)]
        return jnp.where(even_row, after.astype(F32), before.astype(F32))

    def shift(layer, x, y):
        slab = a[layer, x, y].astype(F32)
        up = pltpu.roll(slab, LP - 1, 0)
        down = pltpu.roll(slab, 1, 0)
        b[x, y] = jnp.where(even, up, down).astype(BF)

    def patch(x, y):
        fill = jnp.broadcast_to(halo[x, y + 7 : y + 8, :], (8, W))
        top = b[x, y, 0:8, :].astype(F32)
        b[x, y, 0:8, :] = jnp.where(top_row, fill, top).astype(BF)
        low = b[x, y, LP - 8 : LP, :].astype(F32)
        b[x, y, LP - 8 : LP, :] = jnp.where(low_row, fill, low).astype(BF)

    def shift_own(layer):
        def step(i, carry):
            for y in range(LY):
                shift(layer, i + 1, y + 1)
            return carry

        lax.fori_loop(0, LX, step, 0)

    late_rows = tuple(range(LAST[0], LAST[0] + LAST[1]))

    def finish_own(layer):
        for x in range(LX):
            halo[x + 1, 8:16, :] = merge(r_all, layer, x)
            for y in range(1, LY + 1):
                patch(x + 1, y)

    def finish_y(layer):
        for iy, y in enumerate((0, LY + 1)):
            rows = merge(r_y, layer, iy)
            for x in range(LX):
                halo[x + 1, y + 7 : y + 8, :] = rows[x : x + 1]
                shift(layer, x + 1, y)
                patch(x + 1, y)

    def finish_side(layer, ix):
        x = ix * (LX + 1)
        halo[x, 8:16, :] = merge(r_x, layer, ix)
        halo[x, 7:8, :] = merge(r_xy, layer, ix, 0)[0:1]
        halo[x, 16:17, :] = merge(r_xy, layer, ix, 1)[0:1]
        for y in range(LY + 2):
            if y not in late_rows:
                shift(layer, x, y)
                patch(x, y)

    def finish_late(layer):
        for x in (0, LX + 1):
            for y in late_rows:
                shift(layer, x, y)
                patch(x, y)

    for layer in range(3):

        def sums(places, spans):
            def rows_of(ref, *index):
                return [ref[(*index, pl.ds(low, size), slice(None))] for low, size in spans]

            total = None
            for along_x in range(3):
                for t in range(4):
                    left, right = [], []
                    for x, j in places:
                        left += rows_of(a, layer, x + along_x, t + 2 * j)
                        right += rows_of(b, x + along_x, t + 2 * j)
                    low = weights[layer, 3 * along_x + t] if t < 3 else blank
                    high = weights[layer, 3 * along_x + t - 1] if t > 0 else blank
                    term = jnp.dot(
                        jnp.concatenate([jnp.concatenate(left, axis=0), jnp.concatenate(right, axis=0)], axis=1),
                        jnp.concatenate([low, high], axis=1),
                        preferred_element_type=F32,
                    )
                    total = term if total is None else total + term
            return total

        def emit(total, places, spans):
            depth = sum(size for _, size in spans)
            total = total + bias[layer]
            value = 0.5 * total * (1.0 + lax.erf(total * 0.7071067811865476))
            if layer < 2:
                for k, (x, j) in enumerate(places):
                    for s in range(2):
                        y = 2 * j + s
                        slab = value[k * depth : (k + 1) * depth, s * W : (s + 1) * W]
                        offset = 0
                        for low, size in spans:
                            a[layer + 1, x + 1, y + 1, low : low + size, :] = slab[offset : offset + size].astype(BF)
                            offset += size
                        if spans[0][0] == 0:
                            keep_rows(x, y, (slab[0:1], slab[depth - 1 :]))
            else:
                rounded = value.astype(BF)
                rows = []
                for k in range(len(places)):
                    part = rounded[k * LP : (k + 1) * LP]
                    turned = jnp.concatenate([part[:, :W], part[:, W:]], axis=0).T
                    rows.append(jnp.concatenate([turned[:C], turned[C:]], axis=1))
                merged = jnp.dot(jnp.concatenate(rows, axis=0), gather[...], preferred_element_type=F32)
                for k, (x, j) in enumerate(places):
                    for s in range(2):
                        wide[x, pl.ds(2 * j + s, C, stride=LY), :] = merged[k * C : (k + 1) * C, s * LZ : (s + 1) * LZ]

        def block(*work):
            values = [sums(*item) for item in work]
            for value, item in zip(values, work):
                emit(value, *item)

        outer = corner_of(outer_planes, outer_pairs)
        ends = ((0, 8), (LP - 8, 8))
        shift_own(layer)
        arrive(layer, lambda entry: entry[0][0] == 0)
        finish_own(layer)
        finish_y(layer)
        if layer < 2:
            block((corner_of(inner_planes, outer_pairs), whole))
            launch(layer + 1, 0)
        else:
            block((corner_of(inner_planes, inner_pairs), whole), (corner_of(inner_planes, outer_pairs), whole))
            for x in inner_planes:
                out[0, :, x] = wide[x].reshape(C, LY, LZ).astype(BF)
        arrive(layer, lambda entry: entry[0][0] != 0 and entry[2] != LAST)
        for ix in range(2):
            finish_side(layer, ix)
        if layer < 2:
            block((outer, whole))
            launch(layer + 1, 1)
            arrive(layer, lambda entry: entry[2] == LAST)
            finish_late(layer)
            block((corner_of(range(LX), inner_pairs), ends), (corner_of(outer_planes, inner_pairs), middle))
            launch(layer + 1, 2, 3)
            block((corner_of(inner_planes, inner_pairs), middle))
        else:
            arrive(layer, lambda entry: entry[2] == LAST)
            finish_late(layer)
            block((outer, whole), (corner_of(outer_planes, inner_pairs), whole))
            for x in outer_planes:
                out[0, :, x] = wide[x].reshape(C, LY, LZ).astype(BF)

    for layer in range(3):
        for which in range(len(PLAN)):
            message(layer, which, a, out_rows, in_rows, send, recv).wait_send()


def shards(field, kernel_one, bias_one, kernel_two, bias_two, kernel_three, bias_three):
    hbm = pl.BlockSpec(memory_space=pltpu.HBM)
    operands = (
        field,
        kernel_one,
        kernel_two,
        kernel_three,
        bias_one.reshape(1, C),
        bias_two.reshape(1, C),
        bias_three.reshape(1, C),
    )
    return pl.pallas_call(
        kernel,
        out_shape=jax.ShapeDtypeStruct(field.shape, BF),
        in_specs=[hbm] * 7,
        out_specs=pl.BlockSpec(memory_space=pltpu.VMEM),
        scratch_shapes=[
            pltpu.VMEM((LX, C, LY, LZ), BF),
            pltpu.VMEM((LX, C * LY, LZ), F32),
            pltpu.VMEM((3, 3, 3, 3, C, C), BF),
            pltpu.VMEM((3, 9, 2 * W, W), BF),
            pltpu.VMEM((3, 1, 2 * W), F32),
            pltpu.VMEM((2 * LZ, 2 * W), BF),
            pltpu.VMEM((2 * W, 2 * LZ), BF),
            pltpu.VMEM((3, LX + 2, LY + 2, LP, W), BF),
            pltpu.VMEM((LX + 2, LY + 2, LP, W), BF),
            pltpu.VMEM((3, 2, LX, LY, W), BF),
            pltpu.VMEM((3, 2, 2, LY, W), BF),
            pltpu.VMEM((3, 2, 2, LY, W), BF),
            pltpu.VMEM((3, 2, 2, 2, LY, W), BF),
            pltpu.VMEM((3, 2, LX, LY, W), BF),
            pltpu.VMEM((3, 2, 2, LY, W), BF),
            pltpu.VMEM((3, 2, 2, LY, W), BF),
            pltpu.VMEM((3, 2, 2, 2, LY, W), BF),
            pltpu.VMEM((2, LX, LY, W), F32),
            pltpu.VMEM((2, 2, LY, W), F32),
            pltpu.VMEM((2, 2, 2, LY, W), F32),
            pltpu.VMEM((LX + 2, 24, W), F32),
            pltpu.VMEM((3, 1, C), F32),
            pltpu.SemaphoreType.DMA((3, len(PLAN))),
            pltpu.SemaphoreType.DMA((3, len(PLAN))),
            pltpu.SemaphoreType.DMA((LX,)),
            pltpu.SemaphoreType.DMA((3,)),
            pltpu.SemaphoreType.DMA((3,)),
        ],
        compiler_params=pltpu.CompilerParams(
            collective_id=0, has_side_effects=True, vmem_limit_bytes=48_000_000
        ),
    )(*[pltpu.with_memory_space_constraint(v, pltpu.HBM) for v in operands])


def solution(mesh):
    return jax.shard_map(
        shards,
        mesh=mesh,
        in_specs=(P(None, None, "gx", "gy", "gz"), P(), P(), P(), P(), P(), P()),
        out_specs=P(None, None, "gx", "gy", "gz"),
        check_vma=False,
    )
```

```python
import jax
import jax.numpy as jnp
from jax import lax
from jax.experimental import pallas as pl
from jax.experimental.pallas import tpu as pltpu
from jax.sharding import PartitionSpec as P

MESH = pl.DeviceIdType.MESH
AXES = ("gx", "gy", "gz")
C = 64
W = 2 * C
LX, LY, LP = 4, 8, 64
LZ = 2 * LP
PAIRS = LY // 2
BF = jnp.bfloat16
F32 = jnp.float32
HIGH = {1: 1, -1: 0}


LAST = (4, LY - 6)


def plan():
    both = (-1, 1)
    entries = [((0, dy, 0), 0, (2, LX - 2)) for dy in both]
    entries += [((dx, dy, dz), 1, None) for dx in both for dy in both for dz in both]
    entries += [((0, dy, dz), 1, None) for dy in both for dz in both]
    entries += [((dx, dy, 0), 1, None) for dx in both for dy in both]
    entries += [((0, dy, 0), 1, piece) for dy in both for piece in ((1, 1), (LX, 1))]
    entries += [((dx, 0, 0), 1, (1, 2)) for dx in both]
    entries += [((dx, 0, dz), 2, None) for dx in both for dz in both]
    entries += [((0, 0, dz), 2, None) for dz in both]
    entries += [((dx, 0, 0), 2, (LY - 1, 2)) for dx in both]
    entries += [((dx, 0, 0), 3, piece) for dx in both for piece in ((3, 1), (LY - 2, 1))]
    entries += [((dx, 0, 0), 3, LAST) for dx in both]
    return entries


PLAN = plan()
WAYS = sorted({way for way, _, _ in PLAN})


def neighbour(way):
    ids = []
    for axis, step in zip(AXES, way):
        count = lax.axis_size(axis)
        ids.append(lax.rem(lax.axis_index(axis) + step + count, count))
    return tuple(ids)


def message(layer, which, a, out_rows, in_rows, send, recv):
    (dx, dy, dz), _, piece = PLAN[which]
    if dz == 0:
        near_x = {1: LX, -1: 1}.get(dx)
        far_x = {1: 0, -1: LX + 1}.get(dx)
        near_y = {1: LY, -1: 1}.get(dy)
        far_y = {1: 0, -1: LY + 1}.get(dy)
        if dx == 0:
            near_x = far_x = pl.ds(*piece)
        if dy == 0:
            near_y = far_y = pl.ds(*piece)
        source = a.at[layer, near_x, near_y]
        target = a.at[layer, far_x, far_y]
    else:
        kind = (dx != 0) + 2 * (dy != 0)
        source = out_rows[kind].at[layer, HIGH[dz]]
        target = in_rows[kind].at[layer, HIGH[-dz]]
        for step in (dx, dy):
            if step != 0:
                source = source.at[HIGH[step]]
                target = target.at[HIGH[-step]]
    return pltpu.make_async_remote_copy(
        src_ref=source,
        dst_ref=target,
        send_sem=send.at[layer, which],
        recv_sem=recv.at[layer, which],
        device_id=neighbour((dx, dy, dz)),
        device_id_type=MESH,
    )


def kernel(
    field, k_one, k_two, k_three, b_one, b_two, b_three, out,
    raw, wide, taps, weights, bias, spread, gather, a, b,
    z_all, z_x, z_y, z_xy, r_all, r_x, r_y, r_xy, e_all, e_y, e_xy, halo, thin,
    send, recv, field_sem, tap_sem, bias_sem,
):
    out_rows = (z_all, z_x, z_y, z_xy)
    in_rows = (r_all, r_x, r_y, r_xy)
    barrier = pltpu.get_barrier_semaphore()
    for way in sorted(WAYS, key=lambda w: -sum(map(abs, w))):
        pl.semaphore_signal(barrier, inc=1, device_id=neighbour(way), device_id_type=MESH)
    field_in = [pltpu.make_async_copy(field.at[0, :, x], raw.at[x], field_sem.at[x]) for x in range(LX)]
    taps_in = [pltpu.make_async_copy(k, taps.at[i], tap_sem.at[i]) for i, k in enumerate((k_one, k_two, k_three))]
    for x in (0, LX - 1, *range(1, LX - 1)):
        field_in[x].start()
    bias_in = [pltpu.make_async_copy(v, thin.at[i], bias_sem.at[i]) for i, v in enumerate((b_one, b_two, b_three))]
    for copy in taps_in + bias_in:
        copy.start()

    def one_hot(natural, paired):
        slab, z = natural // LZ, natural % LZ
        parity, other, pair = paired // W, (paired // LP) % 2, paired % LP
        return ((slab == other) & (z == 2 * pair + parity)).astype(F32).astype(BF)

    first = lax.broadcasted_iota(jnp.int32, (2 * LZ, 2 * W), 0)
    second = lax.broadcasted_iota(jnp.int32, (2 * LZ, 2 * W), 1)
    spread[...] = one_hot(first, second)
    gather[...] = one_hot(second, first)

    e_y[...] = jnp.zeros_like(e_y)
    e_xy[...] = jnp.zeros_like(e_xy)

    def keep_rows(x, y, rows):
        for side in range(2):
            e_all[side, x, y : y + 1, :] = rows[side]
            if y in (0, LY - 1):
                e_y[side, y // (LY - 1), x : x + 1, :] = rows[side]
                if x in (0, LX - 1):
                    e_xy[side, x // (LX - 1), y // (LY - 1), 0:1, :] = rows[side]

    def relay_in(x):
        field_in[x].wait()
        wide[x] = raw[x].astype(F32).reshape(C * LY, LZ)
        rows = []
        for j in range(PAIRS):
            pair = [wide[x, pl.ds(2 * j + s, C, stride=LY), :].astype(BF) for s in range(2)]
            rows.append(jnp.concatenate(pair, axis=1))
        split = jnp.dot(jnp.concatenate(rows, axis=0), spread[...], preferred_element_type=F32).astype(BF)
        for j in range(PAIRS):
            block = split[j * C : (j + 1) * C]
            cells = jnp.concatenate([block[:, :W], block[:, W:]], axis=0).T
            for s in range(2):
                y = 2 * j + s
                slab = cells[s * LP : (s + 1) * LP]
                a[0, x + 1, y + 1] = slab
                keep_rows(x, y, (slab[:16].astype(F32)[:1], slab[LP - 16 :].astype(F32)[15:]))

    def pack(layer, stage):
        for side in range(2):
            for i in range(2):
                if stage == 1:
                    for j in range(2):
                        z_xy[layer, side, i, j] = e_xy[side, i, j].astype(BF)
                    z_y[layer, side, i] = e_y[side, i].astype(BF)
                elif stage == 2:
                    z_x[layer, side, i] = e_all[side, i * (LX - 1)].astype(BF)
            if stage == 2:
                for x in range(LX):
                    z_all[layer, side, x] = e_all[side, x].astype(BF)

    def launch(layer, *stages, first=lambda entry: 0):
        for stage in stages:
            pack(layer, stage)
        for which, entry in sorted(enumerate(PLAN), key=lambda item: first(item[1])):
            if entry[1] in stages:
                message(layer, which, a, out_rows, in_rows, send, recv).start()

    def arrive(layer, choose):
        for which, entry in enumerate(PLAN):
            if choose(entry):
                message(layer, which, a, out_rows, in_rows, send, recv).wait_recv()

    outer_planes, inner_planes = (0, LX - 1), tuple(range(1, LX - 1))
    outer_pairs, inner_pairs = (0, PAIRS - 1), tuple(range(1, PAIRS - 1))
    whole, middle = ((0, LP),), ((8, LP - 16),)

    def corner_of(planes, pairs):
        return [(x, j) for x in planes for j in pairs]

    for x in outer_planes:
        relay_in(x)
    for x in inner_planes:
        relay_in(x)
    pl.semaphore_wait(barrier, len(WAYS))
    launch(0, *range(4), first=lambda entry: (entry[0][2] == 0) + (entry[0][1] == 0 and entry[0][2] == 0))

    none = jnp.zeros((C, C), BF)
    for layer in range(3):
        taps_in[layer].wait()
        bias_in[layer].wait()
        twice = jnp.concatenate([thin[layer], thin[layer]], axis=1)
        bias[layer] = jnp.concatenate([twice, twice], axis=1)

        def band(i, carry):
            along_x, along_y = i // 3, i % 3
            tap = [taps[layer, along_x, along_y, f] for f in range(3)]
            order = ((tap[1], tap[0]), (tap[2], tap[1]), (none, tap[2]), (tap[0], none))
            for k, (low, high) in enumerate(order):
                block = jnp.concatenate([low, high], axis=0).T
                weights[layer, i, k * C : (k + 1) * C, :] = block
            return carry

        lax.fori_loop(0, 9, band, 0)

    lane = lax.broadcasted_iota(jnp.int32, (LP, W), 1)
    row = lax.broadcasted_iota(jnp.int32, (LP, W), 0)
    even = lane < C
    top_row = (~even & (row == 0))[:8]
    low_row = (even & (row == LP - 1))[LP - 8 :]
    even_row = lax.broadcasted_iota(jnp.int32, (LY, W), 1) < C
    blank = jnp.zeros((2 * W, W), BF)

    def merge(ref, layer, *index):
        after, before = ref[(layer, 1, *index)], ref[(layer, 0, *index)]
        return jnp.where(even_row, after.astype(F32), before.astype(F32))

    def shift(layer, x, y):
        slab = a[layer, x, y].astype(F32)
        up = pltpu.roll(slab, LP - 1, 0)
        down = pltpu.roll(slab, 1, 0)
        b[x, y] = jnp.where(even, up, down).astype(BF)

    def patch(x, y):
        fill = jnp.broadcast_to(halo[x, y + 7 : y + 8, :], (8, W))
        top = b[x, y, 0:8, :].astype(F32)
        b[x, y, 0:8, :] = jnp.where(top_row, fill, top).astype(BF)
        low = b[x, y, LP - 8 : LP, :].astype(F32)
        b[x, y, LP - 8 : LP, :] = jnp.where(low_row, fill, low).astype(BF)

    def shift_own(layer):
        def step(i, carry):
            for y in range(LY):
                shift(layer, i + 1, y + 1)
            return carry

        lax.fori_loop(0, LX, step, 0)

    late_rows = tuple(range(LAST[0], LAST[0] + LAST[1]))

    def finish_own(layer):
        for x in range(LX):
            halo[x + 1, 8:16, :] = merge(r_all, layer, x)
            for y in range(1, LY + 1):
                patch(x + 1, y)

    def finish_y(layer):
        for iy, y in enumerate((0, LY + 1)):
            rows = merge(r_y, layer, iy)
            for x in range(LX):
                halo[x + 1, y + 7 : y + 8, :] = rows[x : x + 1]
                shift(layer, x + 1, y)
                patch(x + 1, y)

    def finish_side(layer, ix):
        x = ix * (LX + 1)
        halo[x, 8:16, :] = merge(r_x, layer, ix)
        halo[x, 7:8, :] = merge(r_xy, layer, ix, 0)[0:1]
        halo[x, 16:17, :] = merge(r_xy, layer, ix, 1)[0:1]
        for y in range(LY + 2):
            if y not in late_rows:
                shift(layer, x, y)
                patch(x, y)

    def finish_late(layer):
        for x in (0, LX + 1):
            for y in late_rows:
                shift(layer, x, y)
                patch(x, y)

    for layer in range(3):

        def sums(places, spans):
            def rows_of(ref, *index):
                return [ref[(*index, pl.ds(low, size), slice(None))] for low, size in spans]

            total = None
            for along_x in range(3):
                for t in range(4):
                    left, right = [], []
                    for x, j in places:
                        left += rows_of(a, layer, x + along_x, t + 2 * j)
                        right += rows_of(b, x + along_x, t + 2 * j)
                    low = weights[layer, 3 * along_x + t] if t < 3 else blank
                    high = weights[layer, 3 * along_x + t - 1] if t > 0 else blank
                    term = jnp.dot(
                        jnp.concatenate([jnp.concatenate(left, axis=0), jnp.concatenate(right, axis=0)], axis=1),
                        jnp.concatenate([low, high], axis=1),
                        preferred_element_type=F32,
                    )
                    total = term if total is None else total + term
            return total

        def emit(total, places, spans):
            depth = sum(size for _, size in spans)
            total = total + bias[layer]
            value = 0.5 * total * (1.0 + lax.erf(total * 0.7071067811865476))
            if layer < 2:
                for k, (x, j) in enumerate(places):
                    for s in range(2):
                        y = 2 * j + s
                        slab = value[k * depth : (k + 1) * depth, s * W : (s + 1) * W]
                        offset = 0
                        for low, size in spans:
                            a[layer + 1, x + 1, y + 1, low : low + size, :] = slab[offset : offset + size].astype(BF)
                            offset += size
                        if spans[0][0] == 0:
                            keep_rows(x, y, (slab[0:1], slab[depth - 1 :]))
            else:
                rounded = value.astype(BF)
                rows = []
                for k in range(len(places)):
                    part = rounded[k * LP : (k + 1) * LP]
                    turned = jnp.concatenate([part[:, :W], part[:, W:]], axis=0).T
                    rows.append(jnp.concatenate([turned[:C], turned[C:]], axis=1))
                merged = jnp.dot(jnp.concatenate(rows, axis=0), gather[...], preferred_element_type=F32)
                for k, (x, j) in enumerate(places):
                    for s in range(2):
                        wide[x, pl.ds(2 * j + s, C, stride=LY), :] = merged[k * C : (k + 1) * C, s * LZ : (s + 1) * LZ]

        def block(*work):
            values = [sums(*item) for item in work]
            for value, item in zip(values, work):
                emit(value, *item)

        outer = corner_of(outer_planes, outer_pairs)
        ends = ((0, 8), (LP - 8, 8))
        shift_own(layer)
        arrive(layer, lambda entry: entry[0][0] == 0)
        finish_own(layer)
        finish_y(layer)
        if layer < 2:
            block((corner_of(inner_planes, outer_pairs), whole))
            launch(layer + 1, 0)
        else:
            block((corner_of(inner_planes, inner_pairs), whole), (corner_of(inner_planes, outer_pairs), whole))
            for x in inner_planes:
                out[0, :, x] = wide[x].reshape(C, LY, LZ).astype(BF)
        arrive(layer, lambda entry: entry[0][0] != 0 and entry[2] != LAST)
        for ix in range(2):
            finish_side(layer, ix)
        if layer < 2:
            block((outer, whole))
            launch(layer + 1, 1)
            arrive(layer, lambda entry: entry[2] == LAST)
            finish_late(layer)
            block((corner_of(range(LX), inner_pairs), ends), (corner_of(outer_planes, inner_pairs), middle))
            launch(layer + 1, 2, 3)
            block((corner_of(inner_planes, inner_pairs), middle))
        else:
            arrive(layer, lambda entry: entry[2] == LAST)
            finish_late(layer)
            block((outer, whole), (corner_of(outer_planes, inner_pairs), whole))
            for x in outer_planes:
                out[0, :, x] = wide[x].reshape(C, LY, LZ).astype(BF)

    for layer in range(3):
        for which in range(len(PLAN)):
            message(layer, which, a, out_rows, in_rows, send, recv).wait_send()


def shards(field, kernel_one, bias_one, kernel_two, bias_two, kernel_three, bias_three):
    hbm = pl.BlockSpec(memory_space=pltpu.HBM)
    operands = (
        field,
        kernel_one,
        kernel_two,
        kernel_three,
        bias_one.reshape(1, C),
        bias_two.reshape(1, C),
        bias_three.reshape(1, C),
    )
    return pl.pallas_call(
        kernel,
        out_shape=jax.ShapeDtypeStruct(field.shape, BF),
        in_specs=[hbm] * 7,
        out_specs=pl.BlockSpec(memory_space=pltpu.VMEM),
        scratch_shapes=[
            pltpu.VMEM((LX, C, LY, LZ), BF),
            pltpu.VMEM((LX, C * LY, LZ), F32),
            pltpu.VMEM((3, 3, 3, 3, C, C), BF),
            pltpu.VMEM((3, 9, 2 * W, W), BF),
            pltpu.VMEM((3, 1, 2 * W), F32),
            pltpu.VMEM((2 * LZ, 2 * W), BF),
            pltpu.VMEM((2 * W, 2 * LZ), BF),
            pltpu.VMEM((3, LX + 2, LY + 2, LP, W), BF),
            pltpu.VMEM((LX + 2, LY + 2, LP, W), BF),
            pltpu.VMEM((3, 2, LX, LY, W), BF),
            pltpu.VMEM((3, 2, 2, LY, W), BF),
            pltpu.VMEM((3, 2, 2, LY, W), BF),
            pltpu.VMEM((3, 2, 2, 2, LY, W), BF),
            pltpu.VMEM((3, 2, LX, LY, W), BF),
            pltpu.VMEM((3, 2, 2, LY, W), BF),
            pltpu.VMEM((3, 2, 2, LY, W), BF),
            pltpu.VMEM((3, 2, 2, 2, LY, W), BF),
            pltpu.VMEM((2, LX, LY, W), F32),
            pltpu.VMEM((2, 2, LY, W), F32),
            pltpu.VMEM((2, 2, 2, LY, W), F32),
            pltpu.VMEM((LX + 2, 24, W), F32),
            pltpu.VMEM((3, 1, C), F32),
            pltpu.SemaphoreType.DMA((3, len(PLAN))),
            pltpu.SemaphoreType.DMA((3, len(PLAN))),
            pltpu.SemaphoreType.DMA((LX,)),
            pltpu.SemaphoreType.DMA((3,)),
            pltpu.SemaphoreType.DMA((3,)),
        ],
        compiler_params=pltpu.CompilerParams(
            collective_id=0, has_side_effects=True, vmem_limit_bytes=48_000_000
        ),
    )(*[pltpu.with_memory_space_constraint(v, pltpu.HBM) for v in operands])


def solution(mesh):
    return jax.shard_map(
        shards,
        mesh=mesh,
        in_specs=(P(None, None, "gx", "gy", "gz"), P(), P(), P(), P(), P(), P()),
        out_specs=P(None, None, "gx", "gy", "gz"),
        check_vma=False,
    )
```

```python
import jax
import jax.numpy as jnp
from jax import lax
from jax.experimental import pallas as pl
from jax.experimental.pallas import tpu as pltpu
from jax.sharding import PartitionSpec as P

MESH = pl.DeviceIdType.MESH
AXES = ("gx", "gy", "gz")
C = 64
W = 2 * C
LX, LY, LP = 4, 8, 64
LZ = 2 * LP
PAIRS = LY // 2
BF = jnp.bfloat16
F32 = jnp.float32
HIGH = {1: 1, -1: 0}


LAST = (4, LY - 6)


def plan():
    both = (-1, 1)
    entries = [((0, dy, 0), 0, (2, LX - 2)) for dy in both]
    entries += [((dx, dy, dz), 1, None) for dx in both for dy in both for dz in both]
    entries += [((0, dy, dz), 1, None) for dy in both for dz in both]
    entries += [((0, dy, 0), 1, piece) for dy in both for piece in ((1, 1), (LX, 1))]
    entries += [((dx, dy, 0), 1, None) for dx in both for dy in both]
    entries += [((dx, 0, 0), 1, (1, 2)) for dx in both]
    entries += [((dx, 0, dz), 2, None) for dx in both for dz in both]
    entries += [((0, 0, dz), 2, None) for dz in both]
    entries += [((dx, 0, 0), 2, (LY - 1, 2)) for dx in both]
    entries += [((dx, 0, 0), 3, piece) for dx in both for piece in ((3, 1), (LY - 2, 1))]
    entries += [((dx, 0, 0), 3, LAST) for dx in both]
    return entries


PLAN = plan()
WAYS = sorted({way for way, _, _ in PLAN})


def neighbour(way):
    ids = []
    for axis, step in zip(AXES, way):
        count = lax.axis_size(axis)
        ids.append(lax.rem(lax.axis_index(axis) + step + count, count))
    return tuple(ids)


def message(layer, which, a, out_rows, in_rows, send, recv):
    (dx, dy, dz), _, piece = PLAN[which]
    if dz == 0:
        near_x = {1: LX, -1: 1}.get(dx)
        far_x = {1: 0, -1: LX + 1}.get(dx)
        near_y = {1: LY, -1: 1}.get(dy)
        far_y = {1: 0, -1: LY + 1}.get(dy)
        if dx == 0:
            near_x = far_x = pl.ds(*piece)
        if dy == 0:
            near_y = far_y = pl.ds(*piece)
        source = a.at[layer, near_x, near_y]
        target = a.at[layer, far_x, far_y]
    else:
        kind = (dx != 0) + 2 * (dy != 0)
        source = out_rows[kind].at[layer, HIGH[dz]]
        target = in_rows[kind].at[layer, HIGH[-dz]]
        for step in (dx, dy):
            if step != 0:
                source = source.at[HIGH[step]]
                target = target.at[HIGH[-step]]
    return pltpu.make_async_remote_copy(
        src_ref=source,
        dst_ref=target,
        send_sem=send.at[layer, which],
        recv_sem=recv.at[layer, which],
        device_id=neighbour((dx, dy, dz)),
        device_id_type=MESH,
    )


def kernel(
    field, k_one, k_two, k_three, b_one, b_two, b_three, out,
    raw, wide, taps, weights, bias, spread, gather, a, b,
    z_all, z_x, z_y, z_xy, r_all, r_x, r_y, r_xy, e_all, e_y, e_xy, halo, thin,
    send, recv, field_sem, tap_sem, bias_sem,
):
    out_rows = (z_all, z_x, z_y, z_xy)
    in_rows = (r_all, r_x, r_y, r_xy)
    barrier = pltpu.get_barrier_semaphore()
    for way in sorted(WAYS, key=lambda w: -sum(map(abs, w))):
        pl.semaphore_signal(barrier, inc=1, device_id=neighbour(way), device_id_type=MESH)
    field_in = [pltpu.make_async_copy(field.at[0, :, x], raw.at[x], field_sem.at[x]) for x in range(LX)]
    taps_in = [pltpu.make_async_copy(k, taps.at[i], tap_sem.at[i]) for i, k in enumerate((k_one, k_two, k_three))]
    for x in (0, LX - 1, *range(1, LX - 1)):
        field_in[x].start()
    bias_in = [pltpu.make_async_copy(v, thin.at[i], bias_sem.at[i]) for i, v in enumerate((b_one, b_two, b_three))]
    for copy in taps_in + bias_in:
        copy.start()

    def one_hot(natural, paired):
        slab, z = natural // LZ, natural % LZ
        parity, other, pair = paired // W, (paired // LP) % 2, paired % LP
        return ((slab == other) & (z == 2 * pair + parity)).astype(F32).astype(BF)

    first = lax.broadcasted_iota(jnp.int32, (2 * LZ, 2 * W), 0)
    second = lax.broadcasted_iota(jnp.int32, (2 * LZ, 2 * W), 1)
    spread[...] = one_hot(first, second)
    gather[...] = one_hot(second, first)

    e_y[...] = jnp.zeros_like(e_y)
    e_xy[...] = jnp.zeros_like(e_xy)

    def keep_rows(x, y, rows):
        for side in range(2):
            e_all[side, x, y : y + 1, :] = rows[side]
            if y in (0, LY - 1):
                e_y[side, y // (LY - 1), x : x + 1, :] = rows[side]
                if x in (0, LX - 1):
                    e_xy[side, x // (LX - 1), y // (LY - 1), 0:1, :] = rows[side]

    def relay_in(x):
        field_in[x].wait()
        wide[x] = raw[x].astype(F32).reshape(C * LY, LZ)
        rows = []
        for j in range(PAIRS):
            pair = [wide[x, pl.ds(2 * j + s, C, stride=LY), :].astype(BF) for s in range(2)]
            rows.append(jnp.concatenate(pair, axis=1))
        split = jnp.dot(jnp.concatenate(rows, axis=0), spread[...], preferred_element_type=F32).astype(BF)
        for j in range(PAIRS):
            block = split[j * C : (j + 1) * C]
            cells = jnp.concatenate([block[:, :W], block[:, W:]], axis=0).T
            for s in range(2):
                y = 2 * j + s
                slab = cells[s * LP : (s + 1) * LP]
                a[0, x + 1, y + 1] = slab
                keep_rows(x, y, (slab[:16].astype(F32)[:1], slab[LP - 16 :].astype(F32)[15:]))

    def pack(layer, stage):
        for side in range(2):
            for i in range(2):
                if stage == 1:
                    for j in range(2):
                        z_xy[layer, side, i, j] = e_xy[side, i, j].astype(BF)
                    z_y[layer, side, i] = e_y[side, i].astype(BF)
                elif stage == 2:
                    z_x[layer, side, i] = e_all[side, i * (LX - 1)].astype(BF)
            if stage == 2:
                for x in range(LX):
                    z_all[layer, side, x] = e_all[side, x].astype(BF)

    def launch(layer, *stages, first=lambda entry: 0):
        for stage in stages:
            pack(layer, stage)
        for which, entry in sorted(enumerate(PLAN), key=lambda item: first(item[1])):
            if entry[1] in stages:
                message(layer, which, a, out_rows, in_rows, send, recv).start()

    def arrive(layer, choose):
        for which, entry in enumerate(PLAN):
            if choose(entry):
                message(layer, which, a, out_rows, in_rows, send, recv).wait_recv()

    outer_planes, inner_planes = (0, LX - 1), tuple(range(1, LX - 1))
    outer_pairs, inner_pairs = (0, PAIRS - 1), tuple(range(1, PAIRS - 1))
    whole, middle = ((0, LP),), ((8, LP - 16),)

    def corner_of(planes, pairs):
        return [(x, j) for x in planes for j in pairs]

    for x in outer_planes:
        relay_in(x)
    for x in inner_planes:
        relay_in(x)
    pl.semaphore_wait(barrier, len(WAYS))
    launch(0, *range(4), first=lambda entry: (entry[0][2] == 0) + (entry[0][1] == 0 and entry[0][2] == 0))

    none = jnp.zeros((C, C), BF)
    for layer in range(3):
        taps_in[layer].wait()
        bias_in[layer].wait()
        twice = jnp.concatenate([thin[layer], thin[layer]], axis=1)
        bias[layer] = jnp.concatenate([twice, twice], axis=1)

        def band(i, carry):
            along_x, along_y = i // 3, i % 3
            tap = [taps[layer, along_x, along_y, f] for f in range(3)]
            order = ((tap[1], tap[0]), (tap[2], tap[1]), (none, tap[2]), (tap[0], none))
            for k, (low, high) in enumerate(order):
                block = jnp.concatenate([low, high], axis=0).T
                weights[layer, i, k * C : (k + 1) * C, :] = block
            return carry

        lax.fori_loop(0, 9, band, 0)

    lane = lax.broadcasted_iota(jnp.int32, (LP, W), 1)
    row = lax.broadcasted_iota(jnp.int32, (LP, W), 0)
    even = lane < C
    top_row = (~even & (row == 0))[:8]
    low_row = (even & (row == LP - 1))[LP - 8 :]
    even_row = lax.broadcasted_iota(jnp.int32, (LY, W), 1) < C
    blank = jnp.zeros((2 * W, W), BF)

    def merge(ref, layer, *index):
        after, before = ref[(layer, 1, *index)], ref[(layer, 0, *index)]
        return jnp.where(even_row, after.astype(F32), before.astype(F32))

    def shift(layer, x, y):
        slab = a[layer, x, y].astype(F32)
        up = pltpu.roll(slab, LP - 1, 0)
        down = pltpu.roll(slab, 1, 0)
        b[x, y] = jnp.where(even, up, down).astype(BF)

    def patch(x, y):
        fill = jnp.broadcast_to(halo[x, y + 7 : y + 8, :], (8, W))
        top = b[x, y, 0:8, :].astype(F32)
        b[x, y, 0:8, :] = jnp.where(top_row, fill, top).astype(BF)
        low = b[x, y, LP - 8 : LP, :].astype(F32)
        b[x, y, LP - 8 : LP, :] = jnp.where(low_row, fill, low).astype(BF)

    def shift_own(layer):
        def step(i, carry):
            for y in range(LY):
                shift(layer, i + 1, y + 1)
            return carry

        lax.fori_loop(0, LX, step, 0)

    late_rows = tuple(range(LAST[0], LAST[0] + LAST[1]))

    def finish_own(layer):
        for x in range(LX):
            halo[x + 1, 8:16, :] = merge(r_all, layer, x)
            for y in range(1, LY + 1):
                patch(x + 1, y)

    def finish_y(layer):
        for iy, y in enumerate((0, LY + 1)):
            rows = merge(r_y, layer, iy)
            for x in range(LX):
                halo[x + 1, y + 7 : y + 8, :] = rows[x : x + 1]
                shift(layer, x + 1, y)
                patch(x + 1, y)

    def finish_side(layer, ix):
        x = ix * (LX + 1)
        halo[x, 8:16, :] = merge(r_x, layer, ix)
        halo[x, 7:8, :] = merge(r_xy, layer, ix, 0)[0:1]
        halo[x, 16:17, :] = merge(r_xy, layer, ix, 1)[0:1]
        for y in range(LY + 2):
            if y not in late_rows:
                shift(layer, x, y)
                patch(x, y)

    def finish_late(layer):
        for x in (0, LX + 1):
            for y in late_rows:
                shift(layer, x, y)
                patch(x, y)

    for layer in range(3):

        def sums(places, spans):
            def rows_of(ref, *index):
                return [ref[(*index, pl.ds(low, size), slice(None))] for low, size in spans]

            total = None
            for along_x in range(3):
                for t in range(4):
                    left, right = [], []
                    for x, j in places:
                        left += rows_of(a, layer, x + along_x, t + 2 * j)
                        right += rows_of(b, x + along_x, t + 2 * j)
                    low = weights[layer, 3 * along_x + t] if t < 3 else blank
                    high = weights[layer, 3 * along_x + t - 1] if t > 0 else blank
                    term = jnp.dot(
                        jnp.concatenate([jnp.concatenate(left, axis=0), jnp.concatenate(right, axis=0)], axis=1),
                        jnp.concatenate([low, high], axis=1),
                        preferred_element_type=F32,
                    )
                    total = term if total is None else total + term
            return total

        def emit(total, places, spans):
            depth = sum(size for _, size in spans)
            total = total + bias[layer]
            value = 0.5 * total * (1.0 + lax.erf(total * 0.7071067811865476))
            if layer < 2:
                for k, (x, j) in enumerate(places):
                    for s in range(2):
                        y = 2 * j + s
                        slab = value[k * depth : (k + 1) * depth, s * W : (s + 1) * W]
                        offset = 0
                        for low, size in spans:
                            a[layer + 1, x + 1, y + 1, low : low + size, :] = slab[offset : offset + size].astype(BF)
                            offset += size
                        if spans[0][0] == 0:
                            keep_rows(x, y, (slab[0:1], slab[depth - 1 :]))
            else:
                rounded = value.astype(BF)
                rows = []
                for k in range(len(places)):
                    part = rounded[k * LP : (k + 1) * LP]
                    turned = jnp.concatenate([part[:, :W], part[:, W:]], axis=0).T
                    rows.append(jnp.concatenate([turned[:C], turned[C:]], axis=1))
                merged = jnp.dot(jnp.concatenate(rows, axis=0), gather[...], preferred_element_type=F32)
                for k, (x, j) in enumerate(places):
                    for s in range(2):
                        wide[x, pl.ds(2 * j + s, C, stride=LY), :] = merged[k * C : (k + 1) * C, s * LZ : (s + 1) * LZ]

        def block(*work):
            values = [sums(*item) for item in work]
            for value, item in zip(values, work):
                emit(value, *item)

        outer = corner_of(outer_planes, outer_pairs)
        ends = ((0, 8), (LP - 8, 8))
        shift_own(layer)
        arrive(layer, lambda entry: entry[0][0] == 0)
        finish_own(layer)
        finish_y(layer)
        if layer < 2:
            block((corner_of(inner_planes, outer_pairs), whole))
            launch(layer + 1, 0)
        else:
            block((corner_of(inner_planes, inner_pairs), whole), (corner_of(inner_planes, outer_pairs), whole))
            for x in inner_planes:
                out[0, :, x] = wide[x].reshape(C, LY, LZ).astype(BF)
        arrive(layer, lambda entry: entry[0][0] != 0 and entry[2] != LAST)
        for ix in range(2):
            finish_side(layer, ix)
        if layer < 2:
            block((outer, whole))
            launch(layer + 1, 1)
            arrive(layer, lambda entry: entry[2] == LAST)
            finish_late(layer)
            block((corner_of(range(LX), inner_pairs), ends), (corner_of(outer_planes, inner_pairs), middle))
            launch(layer + 1, 2, 3)
            block((corner_of(inner_planes, inner_pairs), middle))
        else:
            arrive(layer, lambda entry: entry[2] == LAST)
            finish_late(layer)
            block((outer, whole), (corner_of(outer_planes, inner_pairs), whole))
            for x in outer_planes:
                out[0, :, x] = wide[x].reshape(C, LY, LZ).astype(BF)

    for layer in range(3):
        for which in range(len(PLAN)):
            message(layer, which, a, out_rows, in_rows, send, recv).wait_send()


def shards(field, kernel_one, bias_one, kernel_two, bias_two, kernel_three, bias_three):
    hbm = pl.BlockSpec(memory_space=pltpu.HBM)
    operands = (
        field,
        kernel_one,
        kernel_two,
        kernel_three,
        bias_one.reshape(1, C),
        bias_two.reshape(1, C),
        bias_three.reshape(1, C),
    )
    return pl.pallas_call(
        kernel,
        out_shape=jax.ShapeDtypeStruct(field.shape, BF),
        in_specs=[hbm] * 7,
        out_specs=pl.BlockSpec(memory_space=pltpu.VMEM),
        scratch_shapes=[
            pltpu.VMEM((LX, C, LY, LZ), BF),
            pltpu.VMEM((LX, C * LY, LZ), F32),
            pltpu.VMEM((3, 3, 3, 3, C, C), BF),
            pltpu.VMEM((3, 9, 2 * W, W), BF),
            pltpu.VMEM((3, 1, 2 * W), F32),
            pltpu.VMEM((2 * LZ, 2 * W), BF),
            pltpu.VMEM((2 * W, 2 * LZ), BF),
            pltpu.VMEM((3, LX + 2, LY + 2, LP, W), BF),
            pltpu.VMEM((LX + 2, LY + 2, LP, W), BF),
            pltpu.VMEM((3, 2, LX, LY, W), BF),
            pltpu.VMEM((3, 2, 2, LY, W), BF),
            pltpu.VMEM((3, 2, 2, LY, W), BF),
            pltpu.VMEM((3, 2, 2, 2, LY, W), BF),
            pltpu.VMEM((3, 2, LX, LY, W), BF),
            pltpu.VMEM((3, 2, 2, LY, W), BF),
            pltpu.VMEM((3, 2, 2, LY, W), BF),
            pltpu.VMEM((3, 2, 2, 2, LY, W), BF),
            pltpu.VMEM((2, LX, LY, W), F32),
            pltpu.VMEM((2, 2, LY, W), F32),
            pltpu.VMEM((2, 2, 2, LY, W), F32),
            pltpu.VMEM((LX + 2, 24, W), F32),
            pltpu.VMEM((3, 1, C), F32),
            pltpu.SemaphoreType.DMA((3, len(PLAN))),
            pltpu.SemaphoreType.DMA((3, len(PLAN))),
            pltpu.SemaphoreType.DMA((LX,)),
            pltpu.SemaphoreType.DMA((3,)),
            pltpu.SemaphoreType.DMA((3,)),
        ],
        compiler_params=pltpu.CompilerParams(
            collective_id=0, has_side_effects=True, vmem_limit_bytes=48_000_000
        ),
    )(*[pltpu.with_memory_space_constraint(v, pltpu.HBM) for v in operands])


def solution(mesh):
    return jax.shard_map(
        shards,
        mesh=mesh,
        in_specs=(P(None, None, "gx", "gy", "gz"), P(), P(), P(), P(), P(), P()),
        out_specs=P(None, None, "gx", "gy", "gz"),
        check_vma=False,
    )
```
